256 devices in a mesh: grp: 4 (over y), dev: 64 (over z, x, core).
Axes of the slice: x: 4, y: 4, z: 8, core: 2. Of those that a mesh axis runs over, the one named last changes fastest.
Arguments:
- nz_user: int32 [32768, 128], P(('grp', 'dev')), may hold values from 0 to 65535
- nz_sub: int32 [32768, 128], P(('grp', 'dev')), may hold values from 0 to 16383
- nz_value: float32 [32768, 128], P(('grp', 'dev')), may hold values from -1 to 1
- tile_word: int32 [32768], P(('grp', 'dev')), may hold values from 0 to 16383, as said below
- word_owner: int32 [16384], replicated, may hold values from 0 to 16383, as said below
- user_factor: bfloat16 [64, 65536], P(None, 'dev'), may hold values from -6 to 6
- sub_factor: bfloat16 [64, 16384], P(None, 'dev'), may hold values from -6 to 6
Outputs:
- word_rows: float32 [64, 16384], P(None, ('grp', 'dev'))
The draws below stay inside these ranges and needn't reach their ends.
Inputs may be any that keep to these rules, and one draw needn't show every extreme that they name: A permutation of the word indices: word w is summed into column word_owner[w] of word_rows. `tile_word`: tile i lies on device i // 128 (grp+dev order). On every device at most 2 tiles belong to words whose output column lies on any one other device, and on every device that bound is reached for some other device.
All inputs are finite; a program needn't handle non-finite values.
Results may differ from the reference program's by a relative error of at most 0.0003.
Values may be sent and summed in bfloat16 or wider, within the bound.
A program may use at most 64 MiB of HBM per device.

```python
import math
import jax
import jax.numpy as jnp
import numpy as np
from jax import lax

RANK = 64
NZ = 128
CAP = 2
TILES_DEV = 128
WORDS_DEV = 64
TILES = 32768
USERS = 65536
SUBS = 16384
WORDS = 16384


def layout(key):
    devices_all = TILES // TILES_DEV
    owner_key = jax.random.fold_in(key, 11)
    word_owner = jax.random.permutation(owner_key, WORDS).astype(jnp.int32)
    word_of_row = jnp.zeros((WORDS,), jnp.int32).at[word_owner].set(jnp.arange(WORDS, dtype=jnp.int32))
    heavy_count = min(4, WORDS_DEV)
    heavy_key = jax.random.fold_in(key, 17)

    def heavy_rows(device_index):
        return jax.random.permutation(jax.random.fold_in(heavy_key, device_index), WORDS_DEV)[:heavy_count].astype(jnp.int32)
    heavy_table = jax.vmap(heavy_rows)(jnp.arange(devices_all, dtype=jnp.int32))

    def one_device(device_index):
        device_key = jax.random.fold_in(jax.random.fold_in(key, 23), device_index)
        key_list = jax.random.split(device_key, 6)
        hot_device = (device_index + 1 + jax.random.randint(key_list[0], (), 0, devices_all - 1)) % devices_all
        pair_ids = jnp.arange(devices_all * CAP, dtype=jnp.int32)
        pair_target = pair_ids // CAP
        order_key = jax.random.permutation(key_list[1], devices_all * CAP).astype(jnp.int32)
        order_key = jnp.where(pair_target == hot_device, -1 - pair_ids % CAP, order_key)
        pair_order = pair_target[jnp.argsort(order_key, stable=True)]
        remote_count = jnp.minimum(jax.random.randint(key_list[2], (), 3 * TILES_DEV // 16, 3 * TILES_DEV // 8 + 1), devices_all * CAP)
        slot_ids = jnp.arange(TILES_DEV, dtype=jnp.int32)
        padded_order = pair_order[jnp.minimum(slot_ids, devices_all * CAP - 1)]
        destination = jnp.where(slot_ids < remote_count, padded_order, device_index).astype(jnp.int32)
        heavy_pick = jax.random.randint(key_list[3], (TILES_DEV,), 0, heavy_count)
        light_pick = jax.random.randint(key_list[4], (TILES_DEV,), 0, WORDS_DEV)
        offset = jnp.where(destination == device_index, light_pick, heavy_table[destination, heavy_pick]).astype(jnp.int32)
        words = word_of_row[destination * WORDS_DEV + offset]
        shuffle = jax.random.permutation(key_list[5], TILES_DEV)
        return words[shuffle].astype(jnp.int32)
    tile_word = jax.vmap(one_device)(jnp.arange(devices_all, dtype=jnp.int32)).reshape(TILES)
    return (word_owner, tile_word)


def draw_word_owner(key, part):
    return layout(key)[0]


def draw_tile_word(key, part):
    return layout(key)[1]


def draw_nz_value(key, part):
    key_list = jax.random.split(jax.random.fold_in(key, 37), 3)
    live_count = jax.random.randint(key_list[0], (TILES, 1), NZ // 4, NZ + 1)
    filled = (jnp.arange(NZ)[None, :] < live_count).astype(jnp.float32)
    raw_values = 0.125 * jax.random.normal(key_list[2], (TILES, NZ))
    return (jnp.clip(raw_values, -1.0, 1.0) * filled).astype(jnp.float32)


def place_ends(result, key, least, high):
    place = [jax.random.randint(jax.random.fold_in(key, axis), (), 0, length) for axis, length in enumerate(result.shape)]
    longest = result.shape.index(max(result.shape))
    next_to = place[:longest] + [(place[longest] + 1) % result.shape[longest]] + place[longest + 1:]
    return result.at[tuple(place)].set(least).at[tuple(next_to)].set(high)


def levels(rng, dims, cuts, least, largest):
    def one(dim, blocks):
        draws = jax.random.uniform(jax.random.fold_in(jax.random.fold_in(rng, 6), dim), (blocks,), jnp.float32, least / len(cuts), largest / len(cuts))
        return jnp.repeat(jnp.exp(draws), dims[dim] // blocks).reshape((-1,) + (1,) * (len(dims) - dim - 1))

    factor_of = one(*cuts[0])
    for cut in cuts[1:]:
        factor_of = factor_of * one(*cut)
    return factor_of


def rank_bounds(amount, slope):
    portions = [(1 << 20) // math.isqrt(standing ** slope) + 1 for standing in range(1, amount + 1)]
    deviation = 1 + sum(portions) // (1 << 30)
    return np.cumsum(np.array([max(1, weight // deviation) for weight in portions]))


def skewed_ids(key, dims, number_of, lean):
    listing = rank_bounds(number_of, lean)
    lot = jax.random.randint(jax.random.fold_in(key, 1), dims, 0, int(listing[number_of - 1]))
    rank = jnp.searchsorted(jnp.asarray(listing, jnp.int32), lot, side="right")
    return jax.random.permutation(jax.random.fold_in(key, 2), number_of)[rank].astype(jnp.int32)


def bell_draw(own_key, shape, deviation, limit, cuts=(), held_as=jnp.bfloat16):
    entries = deviation * jax.random.normal(own_key, shape, jnp.float32)
    if cuts:
        entries = entries * levels(own_key, shape, cuts, -0.22, 0.18)
    return jnp.clip(entries, -limit, limit).astype(held_as)


def setup_inputs(seed: int = 0) -> dict:
    seeds = jax.random.split(jax.random.key(seed), 8)
    return {
        "nz_user": place_ends(jax.random.randint(seeds[0], (TILES, NZ), 0, USERS), jax.random.fold_in(seeds[0], 1), 0, USERS - 1).astype(jnp.int32),
        "nz_sub": place_ends(skewed_ids(seeds[1], (TILES, NZ), SUBS, 2), jax.random.fold_in(seeds[1], 3), 0, SUBS - 1).astype(jnp.int32),
        "nz_value": draw_nz_value(jax.random.fold_in(seeds[7], 71), 0),
        "tile_word": draw_tile_word(jax.random.fold_in(seeds[7], 71), 0),
        "word_owner": draw_word_owner(jax.random.fold_in(seeds[7], 71), 0),
        "user_factor": bell_draw(seeds[5], (RANK, USERS), 1.0, 6.0, ((1, 64),)),
        "sub_factor": bell_draw(seeds[6], (RANK, SUBS), 1.0, 6.0, ((1, 64),)),
    }


def reference(nz_user, nz_sub, nz_value, tile_word, word_owner, user_factor, sub_factor):
    tile_total, tile_width = nz_user.shape
    block_tiles = min(tile_total, 256)
    block_count = tile_total // block_tiles

    def one_block(block_args):
        users_block, subs_block, vals_block = block_args
        user_cols = jnp.take(user_factor, users_block, axis=1).astype(jnp.float32)
        sub_cols = jnp.take(sub_factor, subs_block, axis=1).astype(jnp.float32)
        return jnp.sum(user_cols * sub_cols * vals_block[None], axis=2)

    block_sums = lax.map(one_block, (nz_user.reshape(block_count, block_tiles, tile_width),
                                     nz_sub.reshape(block_count, block_tiles, tile_width),
                                     nz_value.reshape(block_count, block_tiles, tile_width)))
    partial_value = jnp.transpose(block_sums, (1, 0, 2)).reshape(block_sums.shape[1], tile_total)
    out_rows = jnp.take(word_owner, tile_word)
    return jnp.zeros((partial_value.shape[0], WORDS), jnp.float32).at[:, out_rows].add(partial_value)
```

```python
import functools

import jax
import jax.numpy as jnp
from jax import lax
from jax.experimental import pallas as pl
from jax.experimental.pallas import tpu as pltpu
from jax.sharding import PartitionSpec as P

CAP = 2
MESH = pl.DeviceIdType.MESH
NT, NZ, LANES = 128, 128, 128
DEVS = 64
U_ROWS, S_ROWS = 512, 128
STEPS = 32
TILES_STEP = NT // STEPS


def kernel(
    kc_ref, urow_ref, srow_ref, v0_ref, v1_ref, u_in, s_in, out_ref,
    ub, sb, utab, stab, sv, g, kc_s, urow_s, srow_s,
    send_u, send_s, recv_u, recv_s, loc,
):
    grp = lax.axis_index("grp")
    dev = lax.axis_index("dev")
    z, x, core = dev // 8, (dev // 2) % 4, dev % 2
    partner = dev + 1 - 2 * core
    lane = lax.broadcasted_iota(jnp.int32, (128, 128), 1)
    sublane = lax.broadcasted_iota(jnp.int32, (128, 128), 0)

    def at(dz, dx, c):
        return ((z + dz + 8) % 8) * 8 + ((x + dx + 4) % 4) * 2 + c

    local_copies = [
        pltpu.make_async_copy(a, b, loc.at[i])
        for i, (a, b) in enumerate(((kc_ref, kc_s), (srow_ref, srow_s), (urow_ref, urow_s)))
    ]
    for c in local_copies:
        c.start()

    barrier = pltpu.get_barrier_semaphore()
    near = [
        ((z + 1) % 8) * 8 + dev % 8,
        ((z + 7) % 8) * 8 + dev % 8,
        at(0, 1, core),
        at(0, 3, core),
        at(0, 2, core),
        partner,
    ]
    for n in near:
        pl.semaphore_signal(barrier, inc=1, device_id=(grp, n), device_id_type=MESH)
    pl.semaphore_wait(barrier, len(near))

    class Table:
        def __init__(self, own, buf, rows, send, recv, convert):
            self.own, self.buf, self.rows = own, buf, rows
            self.send, self.recv, self.convert = send, recv, convert

        def part(self, d, half):
            rows = self.rows if half is None else self.rows // 2
            first = d * self.rows + (0 if half is None else half * rows)
            return self.buf.at[pl.ds(pl.multiple_of(first, 16), rows), :]

        def put(self, d, to, half=None, own=False):
            dst = self.part(d, half)
            src = self.own if own else dst
            pltpu.make_async_remote_copy(
                src_ref=src, dst_ref=dst, send_sem=self.send,
                recv_sem=self.recv.at[d, 0 if half is None else half],
                device_id=(grp, to), device_id_type=MESH,
            ).start()

        def wait(self, d, half=None):
            ref = self.part(d, half)
            pltpu.make_async_remote_copy(
                src_ref=ref, dst_ref=ref, send_sem=self.send,
                recv_sem=self.recv.at[d, 0 if half is None else half],
                device_id=(grp, partner), device_id_type=MESH,
            ).wait_recv()

        def sent(self):
            ref = self.buf.at[pl.ds(0, 63 * self.rows), :]
            pltpu.make_async_remote_copy(
                src_ref=ref, dst_ref=ref, send_sem=self.send, recv_sem=self.recv.at[0, 0],
                device_id=(grp, partner), device_id_type=MESH,
            ).wait_send()

        def take(self, d):
            base = d * self.rows
            self.convert(self.buf, base, base)

    def convert_u(src, first, row):
        @pl.loop(0, 4)
        def _(i):
            a = pl.multiple_of(first + i * 128, 128)
            b = pl.multiple_of(row + i * 128, 128)
            utab[pl.ds(b, 128), :] = src[pl.ds(a, 128), :].astype(jnp.float32)

    def convert_s(src, first, row):
        v = src[pl.ds(pl.multiple_of(first, 128), 128), :].astype(jnp.float32)
        r = pltpu.roll(v, 64, 1)
        stab[pl.ds(pl.multiple_of(2 * row, 128), 128), :] = jnp.where(lane < 64, v, r)
        stab[pl.ds(pl.multiple_of(2 * row + 128, 128), 128), :] = jnp.where(lane < 64, r, v)

    ut = Table(u_in, ub, U_ROWS, send_u, recv_u, convert_u)
    st = Table(s_in, sb, S_ROWS, send_s, recv_s, convert_s)

    xs = (0, 1, 3, 2)
    zp, zm = near[0], near[1]
    xp, xm = near[2], near[3]

    def f1_own(t):
        for to in (xp, xm, near[4], zp, zm, partner):
            t.put(dev, to, own=True)
        t.convert(t.own, 0, dev * t.rows)

    def f1_x(t, j):
        d = at(0, xs[j], 0)
        t.wait(d)
        for to in (zp, zm, partner):
            t.put(d, to)
        t.take(d)

    def f1_z(t, k, j, s):
        d = at(-k if s == 0 else k, xs[j], 0)
        t.wait(d)
        t.put(d, zp if s == 0 else zm, half=s if k == 3 else None)
        t.put(d, partner)
        t.take(d)

    def f1_last(t, j):
        d = at(4, xs[j], 0)
        t.wait(d, 0)
        t.wait(d, 1)
        t.put(d, partner)
        t.take(d)

    zs = (0, -1, 1, -2, 2, -3, 3, 4)

    def f2_own(t):
        for to in (zp, zm, xp, xm, partner):
            t.put(dev, to, own=True)
        t.convert(t.own, 0, dev * t.rows)

    def f2_z(t, m):
        d = at(zs[m], 0, 1)
        if m == 7:
            t.wait(d, 0)
            t.wait(d, 1)
        else:
            t.wait(d)
            s = (m + 1) % 2
            t.put(d, zp if s == 0 else zm, half=s if m >= 5 else None)
        for to in (xp, xm, partner):
            t.put(d, to)
        t.take(d)

    def f2_x(t, m, s):
        d = at(zs[m], 3 if s == 0 else 1, 1)
        t.wait(d)
        t.put(d, xp if s == 0 else xm, half=s)
        t.put(d, partner)
        t.take(d)

    def f2_x2(t, m):
        d = at(zs[m], 2, 1)
        t.wait(d, 0)
        t.wait(d, 1)
        t.put(d, partner)
        t.take(d)

    def part(f, *a):
        return functools.partial(f, *a)

    def f1_zs(t, k):
        return [part(f1_z, t, k, j, s) for j in range(4) for s in range(2)]

    def f2_xs(t, m):
        return [part(f2_x, t, m, 0), part(f2_x, t, m, 1)]

    x_all = lambda t: [part(f1_x, t, j) for j in (1, 2, 3)]
    early0 = (
        [part(f1_own, st), part(f1_own, ut)]
        + x_all(st) + f1_zs(st, 1) + x_all(ut) + f1_zs(st, 2) + f1_zs(ut, 1) + f1_zs(st, 3)
        + [part(f1_last, st, j) for j in range(4)]
    )
    late0 = f1_zs(ut, 2) + f1_zs(ut, 3) + [part(f1_last, ut, j) for j in range(4)]

    fz = lambda t, *ms: [part(f2_z, t, m) for m in ms]
    fx = lambda t, *ms: sum([f2_xs(t, m) for m in ms], [])
    f2 = lambda t, *ms: [part(f2_x2, t, m) for m in ms]
    early1 = (
        [part(f2_own, st), part(f2_own, ut)]
        + fz(st, 1, 2) + fx(st, 0) + fz(st, 3, 4) + fz(ut, 1, 2) + fx(st, 1, 2) + f2(st, 0)
        + fz(st, 5, 6) + fx(st, 3, 4) + f2(st, 1, 2) + fz(st, 7) + fx(ut, 0) + fz(ut, 3, 4)
        + fx(st, 5, 6) + f2(st, 3, 4) + fx(st, 7) + f2(st, 5, 6, 7)
    )
    late1 = (
        fx(ut, 1, 2) + fz(ut, 5, 6) + f2(ut, 0) + fx(ut, 3, 4) + fz(ut, 7) + f2(ut, 1, 2)
        + fx(ut, 5, 6) + f2(ut, 3, 4) + fx(ut, 7) + f2(ut, 5, 6, 7)
    )

    order0 = [(0, xs[j]) for j in range(4)]
    order0 += [((-k, k)[s], xs[j]) for k in (1, 2, 3) for j in range(4) for s in range(2)]
    order0 += [(4, xs[j]) for j in range(4)]
    order1 = [(0, 0)]

    def walk(events):
        out = []
        for e in events:
            f, a = e.func, e.args
            if a[0] is not ut:
                continue
            if f is f2_z:
                out.append((zs[a[1]], 0))
            elif f is f2_x:
                out.append((zs[a[1]], 3 if a[2] == 0 else 1))
            elif f is f2_x2:
                out.append((zs[a[1]], 2))
        return out

    order1 += walk(early1) + walk(late1)

    def from_partner(t, i, c):
        dz, dx = (order1, order0)[c][i]
        d = at(dz, dx, 1 - c)
        t.wait(d)
        t.take(d)

    for c, events in ((0, early0), (1, early1)):

        @pl.when(core == c)
        def _():
            for e in events:
                e()

    @pl.loop(0, 32)
    def _(i):
        d = i * 2 + 1 - core
        st.wait(d)
        st.take(d)

    for c in local_copies:
        c.wait()
    ks = [kc_s[j] for j in range(8)]

    def phase1(t):
        for n in range(NZ):
            idx = srow_s.at[pl.ds(pl.multiple_of(t * NZ + n // 8 * 8, 8), 8)]
            g[n : n + 1, :] = stab[pl.ds(idx[ks[n % 8]], 1), :]
        a = jnp.broadcast_to(v0_ref[pl.ds(t, 1), :], (128, 128))
        b = jnp.broadcast_to(v1_ref[pl.ds(t, 1), :], (128, 128))
        m = jnp.where(sublane < 64, a, b).T
        sv[pl.ds(pl.multiple_of(t * NZ, 128), 128), :] = g[...] * m

    def phase2(t):
        accs = [jnp.zeros((1, 128), jnp.float32) for _ in range(4)]
        for n in range(NZ):
            idx = urow_s.at[pl.ds(pl.multiple_of(t * NZ + n // 8 * 8, 8), 8)]
            row = utab[pl.ds(idx[ks[n % 8]], 1), :]
            accs[n % 4] = accs[n % 4] + row * sv[pl.ds(t * NZ + n, 1), :]
        out_ref[pl.ds(t, 1), :] = (accs[0] + accs[1]) + (accs[2] + accs[3])

    @pl.loop(0, STEPS)
    def _(i):
        for c, events in ((0, late0), (1, late1)):

            @pl.when(core == c)
            def _():
                for e, event in enumerate(events):
                    pl.when(i == e * STEPS // len(events))(event)
                for e in range(32):
                    pl.when(i == e)(part(from_partner, ut, e, c))

        @pl.loop(0, TILES_STEP)
        def _(j):
            phase1(i * TILES_STEP + j)

    @pl.loop(0, NT)
    def _(t):
        phase2(t)

    st.sent()
    ut.sent()


def tile_sums(user_factor, sub_factor, nz_user, nz_sub, nz_value):
    f32, i32, bf16 = jnp.float32, jnp.int32, jnp.bfloat16
    u_in = jnp.concatenate([user_factor[:, :U_ROWS], user_factor[:, U_ROWS:]], axis=0).T
    s_in = jnp.concatenate([sub_factor[:, :S_ROWS], sub_factor[:, S_ROWS:]], axis=0).T
    urow = (nz_user // (2 * U_ROWS)) * U_ROWS + nz_user % U_ROWS
    upper = (nz_user // U_ROWS) % 2 == 1
    v0 = jnp.where(upper, 0.0, nz_value)
    v1 = jnp.where(upper, nz_value, 0.0)
    kc = jnp.arange(128, dtype=i32)
    vmem = pl.BlockSpec(memory_space=pltpu.VMEM)
    hbm = pl.BlockSpec(memory_space=pl.ANY)
    acc = pl.pallas_call(
        kernel,
        out_shape=jax.ShapeDtypeStruct((NT, LANES), f32),
        in_specs=[hbm, hbm, hbm, vmem, vmem, vmem, vmem],
        out_specs=vmem,
        scratch_shapes=[
            pltpu.VMEM((DEVS * U_ROWS, LANES), bf16),
            pltpu.VMEM((DEVS * S_ROWS, LANES), bf16),
            pltpu.VMEM((DEVS * U_ROWS, LANES), f32),
            pltpu.VMEM((DEVS * S_ROWS * 2, LANES), f32),
            pltpu.VMEM((NT * NZ, LANES), f32),
            pltpu.VMEM((NZ, LANES), f32),
            pltpu.SMEM((128,), i32),
            pltpu.SMEM((NT * NZ,), i32),
            pltpu.SMEM((NT * NZ,), i32),
            pltpu.SemaphoreType.DMA,
            pltpu.SemaphoreType.DMA,
            pltpu.SemaphoreType.DMA((DEVS, 2)),
            pltpu.SemaphoreType.DMA((DEVS, 2)),
            pltpu.SemaphoreType.DMA((3,)),
        ],
        compiler_params=pltpu.CompilerParams(
            collective_id=0, has_side_effects=True, vmem_limit_bytes=58 * 2**20
        ),
    )(kc, urow.reshape(-1), nz_sub.reshape(-1), v0, v1, u_in, s_in)
    return acc[:, :64] + acc[:, 64:]


def cut_along(value, dim, peers):
    shape = value.shape
    pieces = value.reshape(*shape[:dim], peers, shape[dim] // peers, *shape[dim + 1 :])
    return jnp.moveaxis(pieces, dim, 0)


def joined_along(pieces, dim):
    pieces = jnp.moveaxis(pieces, 0, dim)
    shape = pieces.shape
    return pieces.reshape(*shape[:dim], shape[dim] * shape[dim + 1], *shape[dim + 2 :])


def exchange_both(value, axis, axes, splits, concats):
    sizes = [lax.axis_size(a) for a in axes]
    pieces = cut_along(value, splits[0], sizes[0])
    pieces = jnp.moveaxis(cut_along(pieces, splits[1] + 1, sizes[1]), 0, 1)
    inside = pieces.shape[2:]
    pieces = pieces.reshape(-1, *inside)
    pieces = lax.all_to_all(pieces, axis, split_axis=0, concat_axis=0, tiled=True)
    pieces = joined_along(pieces.reshape(*sizes, *inside), concats[0] + 1)
    return joined_along(pieces, concats[1])


def shards(nz_user, nz_sub, nz_value, tile_word, word_owner, user_factor, sub_factor):
    tile_rows = tile_sums(user_factor, sub_factor, nz_user, nz_sub, nz_value)
    tile_count, rank_width = tile_rows.shape
    grp_size = lax.axis_size("grp")
    dev_size = lax.axis_size("dev")
    devices_all = grp_size * dev_size
    words_total = word_owner.shape[0]
    words_local = words_total // devices_all
    out_rows = jnp.take(word_owner, tile_word)
    self_index = lax.axis_index("grp") * dev_size + lax.axis_index("dev")
    owner_dev = out_rows // words_local
    local_row = out_rows - owner_dev * words_local
    owned = owner_dev == self_index
    columns = jnp.arange(words_local, dtype=jnp.int32)
    own_table = (owned[:, None] & (local_row[:, None] == columns[None, :])).astype(jnp.float32)
    own_part = jnp.einsum("tr,tk->rk", tile_rows, own_table, precision=lax.Precision.HIGHEST)
    peer_ids = jnp.arange(devices_all, dtype=jnp.int32)
    outgoing = (jnp.logical_not(owned)[:, None] & (owner_dev[:, None] == peer_ids[None, :])).astype(
        jnp.float32
    )
    tile_ids = jnp.arange(tile_count, dtype=jnp.int32)
    earlier_table = (tile_ids[:, None] > tile_ids[None, :]).astype(jnp.float32)
    earlier = jnp.dot(
        earlier_table, outgoing, precision=lax.Precision.HIGHEST, preferred_element_type=jnp.float32
    )
    position = jnp.sum(earlier * outgoing, axis=1).astype(jnp.int32)
    send_slot = jnp.where(owned, devices_all * CAP, owner_dev * CAP + position)
    slot_ids = jnp.arange(devices_all * CAP, dtype=jnp.int32)
    slot_table = (send_slot[:, None] == slot_ids[None, :]).astype(jnp.float32)
    send_rows = jnp.einsum("ts,tr->sr", slot_table, tile_rows, precision=lax.Precision.HIGHEST)
    filled = jnp.sum(slot_table, axis=0)
    send_ids = (
        jnp.dot(
            local_row.astype(jnp.float32),
            slot_table,
            precision=lax.Precision.HIGHEST,
            preferred_element_type=jnp.float32,
        )
        + filled
        - 1.0
    )
    send_rows = send_rows.reshape(grp_size, dev_size, CAP * rank_width)
    send_ids = send_ids.reshape(grp_size, dev_size, CAP)
    got_rows, got_ids = (
        exchange_both(send_rows, ("dev", "grp"), ("dev", "grp"), (1, 0), (1, 0)),
        exchange_both(send_ids, ("dev", "grp"), ("dev", "grp"), (1, 0), (1, 0)),
    )
    got_rows = got_rows.reshape(devices_all * CAP, rank_width)
    got_ids = got_ids.reshape(devices_all * CAP).astype(jnp.int32)
    got_table = (got_ids[:, None] == columns[None, :]).astype(jnp.float32)
    far_part = jnp.einsum("sr,sk->rk", got_rows, got_table, precision=lax.Precision.HIGHEST)
    return own_part + far_part


def solution(mesh):
    return jax.shard_map(
        shards,
        mesh=mesh,
        in_specs=(
            P(("grp", "dev"), None),
            P(("grp", "dev"), None),
            P(("grp", "dev"), None),
            P(("grp", "dev")),
            P(),
            P(None, "dev"),
            P(None, "dev"),
        ),
        out_specs=P(None, ("grp", "dev")),
        check_vma=False,
    )
```

```python
import functools

import jax
import jax.numpy as jnp
from jax import lax
from jax.experimental import pallas as pl
from jax.experimental.pallas import tpu as pltpu
from jax.sharding import PartitionSpec as P

CAP = 2
MESH = pl.DeviceIdType.MESH
NT, NZ, LANES = 128, 128, 128
DEVS = 64
U_ROWS, S_ROWS = 512, 128
STEPS = 32
TILES_STEP = NT // STEPS


def kernel(
    kc_ref, word_ref, owner_ref, srow_ref, user_ref, value_ref, uf_ref, sf_ref, out_ref,
    ub, sb, utab, stab, sv, g, u_in, s_in, urow_v, v0_ref, v1_ref, sums,
    id_out, id_mid, id_turn, id_in, row_out, row_mid, row_turn, row_in, slots,
    kc_s, word_s, owner_s, urow_s, srow_s,
    send_u, send_s, recv_u, recv_s, loc, send_x, recv_x,
):
    grp = lax.axis_index("grp")
    dev = lax.axis_index("dev")
    z, x, core = dev // 8, (dev // 2) % 4, dev % 2
    partner = dev + 1 - 2 * core
    lane = lax.broadcasted_iota(jnp.int32, (128, 128), 1)
    sublane = lax.broadcasted_iota(jnp.int32, (128, 128), 0)

    def at(dz, dx, c):
        return ((z + dz + 8) % 8) * 8 + ((x + dx + 4) % 4) * 2 + c

    me = grp * DEVS + dev
    quad = grp * 8 + dev % 8

    def in_plane(q):
        return (q // 8, z * 8 + q % 8)

    pairs = ((word_ref, word_s), (owner_ref, owner_s), (kc_ref, kc_s), (srow_ref, srow_s))
    local_copies = [pltpu.make_async_copy(a, b, loc.at[i]) for i, (a, b) in enumerate(pairs)]
    for c in local_copies:
        c.start()

    for src, dst, rows in ((uf_ref, u_in, U_ROWS), (sf_ref, s_in, S_ROWS)):
        for i in range(rows // 128):
            a = src[:, i * 128 : (i + 1) * 128].astype(jnp.float32)
            b = src[:, rows + i * 128 : rows + (i + 1) * 128].astype(jnp.float32)
            t = jnp.concatenate([a, b], axis=0).T
            dst[i * 128 : (i + 1) * 128, :] = t.astype(jnp.bfloat16)

    users = user_ref[...]
    urow_v[...] = (users // (2 * U_ROWS)) * U_ROWS + users % U_ROWS
    upper = (users // U_ROWS) % 2 == 1
    v0_ref[...] = jnp.where(upper, 0.0, value_ref[...])
    v1_ref[...] = jnp.where(upper, value_ref[...], 0.0)

    barrier = pltpu.get_barrier_semaphore()
    near = [
        ((z + 1) % 8) * 8 + dev % 8,
        ((z + 7) % 8) * 8 + dev % 8,
        at(0, 1, core),
        at(0, 3, core),
        at(0, 2, core),
        partner,
    ]
    for i in range(1, 8):
        to = ((z + i) % 8) * 8 + dev % 8
        pl.semaphore_signal(barrier, inc=1, device_id=(grp, to), device_id_type=MESH)
    for i in range(1, 32):
        to = in_plane((quad + i) % 32)
        pl.semaphore_signal(barrier, inc=1, device_id=to, device_id_type=MESH)
    pl.semaphore_wait(barrier, 38)

    copy_u = pltpu.make_async_copy(urow_v, urow_s, loc.at[4])
    copy_u.start()
    local_copies.append(copy_u)

    class Table:
        def __init__(self, own, buf, rows, send, recv, convert):
            self.own, self.buf, self.rows = own, buf, rows
            self.send, self.recv, self.convert = send, recv, convert

        def part(self, d, half):
            rows = self.rows if half is None else self.rows // 2
            first = d * self.rows + (0 if half is None else half * rows)
            return self.buf.at[pl.ds(pl.multiple_of(first, 16), rows), :]

        def put(self, d, to, half=None, own=False):
            dst = self.part(d, half)
            src = self.own if own else dst
            pltpu.make_async_remote_copy(
                src_ref=src, dst_ref=dst, send_sem=self.send,
                recv_sem=self.recv.at[d, 0 if half is None else half],
                device_id=(grp, to), device_id_type=MESH,
            ).start()

        def wait(self, d, half=None):
            ref = self.part(d, half)
            pltpu.make_async_remote_copy(
                src_ref=ref, dst_ref=ref, send_sem=self.send,
                recv_sem=self.recv.at[d, 0 if half is None else half],
                device_id=(grp, partner), device_id_type=MESH,
            ).wait_recv()

        def sent(self):
            ref = self.buf.at[pl.ds(0, 63 * self.rows), :]
            pltpu.make_async_remote_copy(
                src_ref=ref, dst_ref=ref, send_sem=self.send, recv_sem=self.recv.at[0, 0],
                device_id=(grp, partner), device_id_type=MESH,
            ).wait_send()

        def take(self, d):
            base = d * self.rows
            self.convert(self.buf, base, base)

    def convert_u(src, first, row):
        @pl.loop(0, 4)
        def _(i):
            a = pl.multiple_of(first + i * 128, 128)
            b = pl.multiple_of(row + i * 128, 128)
            utab[pl.ds(b, 128), :] = src[pl.ds(a, 128), :].astype(jnp.float32)

    def convert_s(src, first, row):
        v = src[pl.ds(pl.multiple_of(first, 128), 128), :].astype(jnp.float32)
        r = pltpu.roll(v, 64, 1)
        stab[pl.ds(pl.multiple_of(2 * row, 128), 128), :] = jnp.where(lane < 64, v, r)
        stab[pl.ds(pl.multiple_of(2 * row + 128, 128), 128), :] = jnp.where(lane < 64, r, v)

    ut = Table(u_in, ub, U_ROWS, send_u, recv_u, convert_u)
    st = Table(s_in, sb, S_ROWS, send_s, recv_s, convert_s)

    xs = (0, 1, 3, 2)
    zp, zm = near[0], near[1]
    xp, xm = near[2], near[3]

    def f1_own(t):
        for to in (xp, xm, near[4], zp, zm, partner):
            t.put(dev, to, own=True)
        t.convert(t.own, 0, dev * t.rows)

    def f1_x(t, j):
        d = at(0, xs[j], 0)
        t.wait(d)
        for to in (zp, zm, partner):
            t.put(d, to)
        t.take(d)

    def f1_z(t, k, j, s):
        d = at(-k if s == 0 else k, xs[j], 0)
        t.wait(d)
        t.put(d, zp if s == 0 else zm, half=s if k == 3 else None)
        t.put(d, partner)
        t.take(d)

    def f1_last(t, j):
        d = at(4, xs[j], 0)
        t.wait(d, 0)
        t.wait(d, 1)
        t.put(d, partner)
        t.take(d)

    zs = (0, -1, 1, -2, 2, -3, 3, 4)

    def f2_own(t):
        for to in (zp, zm, xp, xm, partner):
            t.put(dev, to, own=True)
        t.convert(t.own, 0, dev * t.rows)

    def f2_z(t, m):
        d = at(zs[m], 0, 1)
        if m == 7:
            t.wait(d, 0)
            t.wait(d, 1)
        else:
            t.wait(d)
            s = (m + 1) % 2
            t.put(d, zp if s == 0 else zm, half=s if m >= 5 else None)
        for to in (xp, xm, partner):
            t.put(d, to)
        t.take(d)

    def f2_x(t, m, s):
        d = at(zs[m], 3 if s == 0 else 1, 1)
        t.wait(d)
        t.put(d, xp if s == 0 else xm, half=s)
        t.put(d, partner)
        t.take(d)

    def f2_x2(t, m):
        d = at(zs[m], 2, 1)
        t.wait(d, 0)
        t.wait(d, 1)
        t.put(d, partner)
        t.take(d)

    def part(f, *a):
        return functools.partial(f, *a)

    def f1_zs(t, k):
        return [part(f1_z, t, k, j, s) for j in range(4) for s in range(2)]

    def f2_xs(t, m):
        return [part(f2_x, t, m, 0), part(f2_x, t, m, 1)]

    x_all = lambda t: [part(f1_x, t, j) for j in (1, 2, 3)]
    early0 = (
        [part(f1_own, st), part(f1_own, ut)]
        + x_all(st) + f1_zs(st, 1) + x_all(ut) + f1_zs(st, 2) + f1_zs(ut, 1) + f1_zs(st, 3)
        + [part(f1_last, st, j) for j in range(4)]
    )
    late0 = f1_zs(ut, 2) + f1_zs(ut, 3) + [part(f1_last, ut, j) for j in range(4)]

    fz = lambda t, *ms: [part(f2_z, t, m) for m in ms]
    fx = lambda t, *ms: sum([f2_xs(t, m) for m in ms], [])
    f2 = lambda t, *ms: [part(f2_x2, t, m) for m in ms]
    early1 = (
        [part(f2_own, st), part(f2_own, ut)]
        + fz(st, 1, 2) + fx(st, 0) + fz(st, 3, 4) + fz(ut, 1, 2) + fx(st, 1, 2) + f2(st, 0)
        + fz(st, 5, 6) + fx(st, 3, 4) + f2(st, 1, 2) + fz(st, 7) + fx(ut, 0) + fz(ut, 3, 4)
        + fx(st, 5, 6) + f2(st, 3, 4) + fx(st, 7) + f2(st, 5, 6, 7)
    )
    late1 = (
        fx(ut, 1, 2) + fz(ut, 5, 6) + f2(ut, 0) + fx(ut, 3, 4) + fz(ut, 7) + f2(ut, 1, 2)
        + fx(ut, 5, 6) + f2(ut, 3, 4) + fx(ut, 7) + f2(ut, 5, 6, 7)
    )

    order0 = [(0, xs[j]) for j in range(4)]
    order0 += [((-k, k)[s], xs[j]) for k in (1, 2, 3) for j in range(4) for s in range(2)]
    order0 += [(4, xs[j]) for j in range(4)]
    order1 = [(0, 0)]

    def walk(events):
        out = []
        for e in events:
            f, a = e.func, e.args
            if a[0] is not ut:
                continue
            if f is f2_z:
                out.append((zs[a[1]], 0))
            elif f is f2_x:
                out.append((zs[a[1]], 3 if a[2] == 0 else 1))
            elif f is f2_x2:
                out.append((zs[a[1]], 2))
        return out

    order1 += walk(early1) + walk(late1)

    def from_partner(t, i, c):
        dz, dx = (order1, order0)[c][i]
        d = at(dz, dx, 1 - c)
        t.wait(d)
        t.take(d)

    def x_copy(src, dst, way, to):
        return pltpu.make_async_remote_copy(
            src_ref=src, dst_ref=dst, send_sem=send_x.at[way], recv_sem=recv_x.at[way],
            device_id=to, device_id_type=MESH,
        )

    def x_first(out, mid, way):
        for i in range(1, 8):
            zt = (z + i) % 8
            src = out.at[pl.ds(pl.multiple_of(zt * 32, 32), 32), :]
            dst = mid.at[pl.ds(pl.multiple_of(z * 40, 8), 32), :]
            x_copy(src, dst, way, (grp, zt * 8 + dev % 8)).start()
        mid[pl.ds(pl.multiple_of(z * 40, 8), 32), :] = out[pl.ds(pl.multiple_of(z * 32, 32), 32), :]

    def x_wait(buf, rows, way):
        ref = buf.at[pl.ds(0, rows), :]
        x_copy(ref, ref, way, (grp, partner)).wait_recv()

    def x_second(mid, turn, into, way):
        x_wait(mid, 224, way)
        for q in range(32):
            turn[q * 8 : q * 8 + 8, :] = mid[pl.ds(q, 8, stride=40), :]
        for i in range(1, 32):
            q = (quad + i) % 32
            src = turn.at[pl.ds(pl.multiple_of(q * 8, 8), 8), :]
            dst = into.at[pl.ds(pl.multiple_of(quad * 8, 8), 8), :]
            x_copy(src, dst, way + 1, in_plane(q)).start()
        own = pl.ds(pl.multiple_of(quad * 8, 8), 8)
        into[own, :] = turn[own, :]

    def x_sent(buf, way):
        for w, rows in ((way, 224), (way + 1, 248)):
            ref = buf.at[pl.ds(0, rows), :]
            x_copy(ref, ref, w, (grp, partner)).wait_send()

    def routing():
        local_copies[0].wait()
        local_copies[1].wait()
        lane1 = lax.broadcasted_iota(jnp.int32, (1, 128), 1)

        def look(i, row):
            for j in range(8):
                t = i * 8 + j
                row = jnp.where(lane1 == t, owner_s[word_s[t]], row)
            return row

        row = lax.fori_loop(0, NT // 8, look, jnp.zeros((1, 128), jnp.int32))
        across = jnp.broadcast_to(row, (128, 128))
        down = across.T
        same = (down // 64 == across // 64) & (sublane < lane)
        place = jnp.sum(same.astype(jnp.float32), axis=0, keepdims=True)
        owner = row // 64
        to = (owner // 8) % 8 * 32 + owner // 64 * 8 + owner % 8
        dest = lax.broadcasted_iota(jnp.int32, (256, 128), 0)
        far = owner != me
        ids = (down % 64 + 1).astype(jnp.bfloat16)
        found = []
        for p in range(CAP):
            hit = (to == dest) & far & (place == p)
            table = hit.astype(jnp.float32).astype(jnp.bfloat16)
            slots[p * 256 : (p + 1) * 256, :] = table
            found.append(jnp.dot(table, ids, preferred_element_type=jnp.float32))
        lane_w = lax.broadcasted_iota(jnp.int32, (256, 128), 1)
        id_out[...] = jnp.where(lane_w < 64, found[0], found[1]) - 1.0
        own = (down // 64 == me) & (down % 64 == lane)
        slots[512:640, :] = own.astype(jnp.float32).astype(jnp.bfloat16)

    def thirds(v):
        hi = v.astype(jnp.bfloat16)
        rest = v - hi.astype(jnp.float32)
        mid = rest.astype(jnp.bfloat16)
        low = (rest - mid.astype(jnp.float32)).astype(jnp.bfloat16)
        return hi, mid, low

    for c, events in ((0, early0), (1, early1)):

        @pl.when(core == c)
        def _():
            for e in events[:2]:
                e()

    routing()
    x_first(id_out, id_mid, 0)

    for c, events in ((0, early0), (1, early1)):

        @pl.when(core == c)
        def _():
            for e in events[2:]:
                e()

    x_second(id_mid, id_turn, id_in, 0)

    @pl.loop(0, 32)
    def _(i):
        d = i * 2 + 1 - core
        st.wait(d)
        st.take(d)

    for c in local_copies[2:]:
        c.wait()
    ks = [kc_s[j] for j in range(8)]

    def phase1(t):
        for n in range(NZ):
            idx = srow_s.at[pl.ds(t, 1), pl.ds(n // 8 * 8, 8)]
            g[n : n + 1, :] = stab[pl.ds(idx[0, ks[n % 8]], 1), :]
        a = jnp.broadcast_to(v0_ref[pl.ds(t, 1), :], (128, 128))
        b = jnp.broadcast_to(v1_ref[pl.ds(t, 1), :], (128, 128))
        m = jnp.where(sublane < 64, a, b).T
        sv[pl.ds(pl.multiple_of(t * NZ, 128), 128), :] = g[...] * m

    def phase2(t):
        accs = [jnp.zeros((1, 128), jnp.float32) for _ in range(4)]
        for n in range(NZ):
            idx = urow_s.at[pl.ds(t, 1), pl.ds(n // 8 * 8, 8)]
            row = utab[pl.ds(idx[0, ks[n % 8]], 1), :]
            accs[n % 4] = accs[n % 4] + row * sv[pl.ds(t * NZ + n, 1), :]
        sums[pl.ds(t, 1), :] = (accs[0] + accs[1]) + (accs[2] + accs[3])

    @pl.loop(0, STEPS)
    def _(i):
        for c, events in ((0, late0), (1, late1)):

            @pl.when(core == c)
            def _():
                for e, event in enumerate(events):
                    pl.when(i == e * STEPS // len(events))(event)
                for e in range(32):
                    pl.when(i == e)(part(from_partner, ut, e, c))

        @pl.loop(0, TILES_STEP)
        def _(j):
            phase1(i * TILES_STEP + j)

    @pl.loop(0, NT)
    def _(t):
        phase2(t)

    total = sums[...]
    total = total + pltpu.roll(total, 64, 1)
    parts = thirds(total)
    lane_w = lax.broadcasted_iota(jnp.int32, (256, 128), 1)
    picked = []
    for p in range(CAP):
        table = slots[p * 256 : (p + 1) * 256, :]
        hi, mid, low = (jnp.dot(table, v, preferred_element_type=jnp.float32) for v in parts)
        picked.append((hi + mid) + low)
    row_out[...] = jnp.where(lane_w < 64, picked[0], picked[1])
    x_first(row_out, row_mid, 2)

    def collect(table, v):
        hi, mid, low = (
            lax.dot_general(w, table, (((0,), (0,)), ((), ())), preferred_element_type=jnp.float32)
            for w in thirds(v)
        )
        return (hi + mid) + low

    own_part = collect(slots[512:640, :], total)
    x_wait(id_in, 248, 1)
    hits = (id_in[...] == (lane_w % 64).astype(jnp.float32)).astype(jnp.float32).astype(jnp.bfloat16)
    st.sent()
    ut.sent()
    x_sent(id_out, 0)
    x_second(row_mid, row_turn, row_in, 2)
    x_wait(row_in, 248, 3)
    far_part = collect(hits, row_in[...])
    out_ref[...] = (own_part[:64, :64] + far_part[:64, :64]) + far_part[64:, 64:]
    x_sent(row_out, 2)


def shards(nz_user, nz_sub, nz_value, tile_word, word_owner, user_factor, sub_factor):
    f32, i32, bf16 = jnp.float32, jnp.int32, jnp.bfloat16
    kc = jnp.arange(128, dtype=i32)
    vmem = pl.BlockSpec(memory_space=pltpu.VMEM)
    hbm = pl.BlockSpec(memory_space=pl.ANY)
    rows = pltpu.VMEM((256, LANES), f32)
    return pl.pallas_call(
        kernel,
        out_shape=jax.ShapeDtypeStruct((64, 64), f32),
        in_specs=[hbm, hbm, hbm, hbm, vmem, vmem, vmem, vmem],
        out_specs=vmem,
        scratch_shapes=[
            pltpu.VMEM((DEVS * U_ROWS, LANES), bf16),
            pltpu.VMEM((DEVS * S_ROWS, LANES), bf16),
            pltpu.VMEM((DEVS * U_ROWS, LANES), f32),
            pltpu.VMEM((DEVS * S_ROWS * 2, LANES), f32),
            pltpu.VMEM((NT * NZ, LANES), f32),
            pltpu.VMEM((NZ, LANES), f32),
            pltpu.VMEM((U_ROWS, LANES), bf16),
            pltpu.VMEM((S_ROWS, LANES), bf16),
            pltpu.VMEM((NT, NZ), i32),
            pltpu.VMEM((NT, NZ), f32),
            pltpu.VMEM((NT, NZ), f32),
            pltpu.VMEM((NT, LANES), f32),
            rows, pltpu.VMEM((320, LANES), f32), rows, rows,
            rows, pltpu.VMEM((320, LANES), f32), rows, rows,
            pltpu.VMEM((640, LANES), bf16),
            pltpu.SMEM((128,), i32),
            pltpu.SMEM((NT,), i32),
            pltpu.SMEM((16384,), i32),
            pltpu.SMEM((NT, NZ), i32),
            pltpu.SMEM((NT, NZ), i32),
            pltpu.SemaphoreType.DMA,
            pltpu.SemaphoreType.DMA,
            pltpu.SemaphoreType.DMA((DEVS, 2)),
            pltpu.SemaphoreType.DMA((DEVS, 2)),
            pltpu.SemaphoreType.DMA((5,)),
            pltpu.SemaphoreType.DMA((4,)),
            pltpu.SemaphoreType.DMA((4,)),
        ],
        compiler_params=pltpu.CompilerParams(
            collective_id=0, has_side_effects=True, vmem_limit_bytes=58 * 2**20
        ),
    )(kc, tile_word, word_owner, nz_sub, nz_user, nz_value, user_factor, sub_factor)


def solution(mesh):
    return jax.shard_map(
        shards,
        mesh=mesh,
        in_specs=(
            P(("grp", "dev"), None),
            P(("grp", "dev"), None),
            P(("grp", "dev"), None),
            P(("grp", "dev")),
            P(),
            P(None, "dev"),
            P(None, "dev"),
        ),
        out_specs=P(None, ("grp", "dev")),
        check_vma=False,
    )
```

```python
import functools

import jax
import jax.numpy as jnp
from jax import lax
from jax.experimental import pallas as pl
from jax.experimental.pallas import tpu as pltpu
from jax.sharding import PartitionSpec as P

CAP = 2
MESH = pl.DeviceIdType.MESH
NT, NZ, LANES = 128, 128, 128
DEVS = 64
U_ROWS, S_ROWS = 512, 128
ROWS = U_ROWS + S_ROWS
SIDE = (288, 160)
LAG_Y, LAG_PARTNER = 6, 8
ORDER = (
    (("x", 0, 1), ("x", 0, 3), ("z", -1, 0), ("z", 1, 0), ("x", 0, 2), ("z", -1, 1), ("z", 1, 1), ("z", -1, 3))
    + (("z", 1, 3), ("z", -2, 0), ("z", 2, 0), ("z", -1, 2), ("z", 1, 2), ("z", -2, 1), ("z", 2, 1), ("z", -2, 3))
    + (("z", 2, 3), ("z", -3, 0), ("z", 3, 0), ("z", -2, 2), ("z", 2, 2), ("z", -3, 1), ("z", 3, 1), ("z", -3, 3))
    + (("z", 3, 3), ("end", 4, 0), ("z", -3, 2), ("z", 3, 2), ("end", 4, 1), ("end", 4, 3), ("end", 4, 2)),
    (("z", -1, 0), ("z", 1, 0), ("x", 0, 1), ("x", 0, 3), ("x", -1, 1), ("x", -1, 3), ("z", -2, 0), ("x", 1, 1))
    + (("z", 2, 0), ("x", 1, 3), ("end", 0, 2), ("end", -1, 2), ("x", -2, 1), ("x", -2, 3), ("z", -3, 0), ("x", 2, 3))
    + (("z", 3, 0), ("x", 2, 1), ("end", 1, 2), ("end", -2, 2), ("x", -3, 3), ("x", -3, 1), ("end", 4, 0), ("x", 3, 1))
    + (("end", 2, 2), ("x", 3, 3), ("end", -3, 2), ("x", 4, 3), ("x", 4, 1), ("end", 3, 2), ("end", 4, 2)),
)


def kernel(
    kc_ref, word_ref, owner_ref, srow_ref, user_ref, value_ref, uf_ref, sf_ref, out_ref,
    buf, utab, stab, sv, g, own_in, urow_v, v0_ref, v1_ref, sums,
    id_out, id_mid, id_turn, id_in, row_out, row_mid, row_turn, row_in, slots,
    kc_s, word_s, owner_s, urow_s, srow_s,
    send_t, recv_t, loc, send_x, recv_x,
):
    grp = lax.axis_index("grp")
    dev = lax.axis_index("dev")
    z, x, core = dev // 8, (dev // 2) % 4, dev % 2
    partner = dev + 1 - 2 * core
    lane = lax.broadcasted_iota(jnp.int32, (128, 128), 1)
    sublane = lax.broadcasted_iota(jnp.int32, (128, 128), 0)

    def at(dz, dx, c):
        return ((z + dz + 8) % 8) * 8 + ((x + dx + 4) % 4) * 2 + c

    me = grp * DEVS + dev
    quad = grp * 8 + dev % 8

    def in_plane(q):
        return (q // 8, z * 8 + q % 8)

    pairs = ((word_ref, word_s), (owner_ref, owner_s), (kc_ref, kc_s), (srow_ref, srow_s))
    local_copies = [pltpu.make_async_copy(a, b, loc.at[i]) for i, (a, b) in enumerate(pairs)]
    for c in local_copies:
        c.start()

    for src, first, rows in ((uf_ref, 0, U_ROWS), (sf_ref, U_ROWS, S_ROWS)):
        for i in range(rows // 128):
            a = src[:, i * 128 : (i + 1) * 128].astype(jnp.float32)
            b = src[:, rows + i * 128 : rows + (i + 1) * 128].astype(jnp.float32)
            t = jnp.concatenate([a, b], axis=0).T
            own_in[first + i * 128 : first + (i + 1) * 128, :] = t.astype(jnp.bfloat16)

    users = user_ref[...]
    urow_v[...] = (users // (2 * U_ROWS)) * U_ROWS + users % U_ROWS
    upper = (users // U_ROWS) % 2 == 1
    v0_ref[...] = jnp.where(upper, 0.0, value_ref[...])
    v1_ref[...] = jnp.where(upper, value_ref[...], 0.0)

    barrier = pltpu.get_barrier_semaphore()
    for i in range(1, 8):
        to = ((z + i) % 8) * 8 + dev % 8
        pl.semaphore_signal(barrier, inc=1, device_id=(grp, to), device_id_type=MESH)
    for i in range(1, 32):
        to = in_plane((quad + i) % 32)
        pl.semaphore_signal(barrier, inc=1, device_id=to, device_id_type=MESH)
    pl.semaphore_wait(barrier, 38)

    copy_u = pltpu.make_async_copy(urow_v, urow_s, loc.at[4])
    copy_u.start()
    local_copies.append(copy_u)

    par = grp % 2
    y_up, y_down = (grp + 1) % 4, (grp + 3) % 4
    zp, zm, xp, xm = at(1, 0, core), at(-1, 0, core), at(0, 1, core), at(0, 3, core)
    x_far = at(0, 2, core)
    sent_rows = [0, 0]

    def shard(d, first, rows):
        return buf.at[pl.ds(pl.multiple_of(d * ROWS + first, 16), rows), :]

    def ring_rows(c, half=None):
        rows = ROWS - SIDE[c]
        first = par * SIDE[c]
        return (first, rows) if half is None else (first + half * (rows // 2), rows // 2)

    def copy(d, first, rows, sem, to, own=False):
        dst = shard(d, first, rows)
        src = own_in.at[pl.ds(pl.multiple_of(first, 16), rows), :] if own else dst
        return pltpu.make_async_remote_copy(
            src_ref=src, dst_ref=dst, send_sem=send_t, recv_sem=recv_t.at[d, sem],
            device_id=to, device_id_type=MESH,
        )

    def put(c, d, span, sem, to, own=False):
        copy(d, *span, sem, to, own).start()
        sent_rows[c] += span[1]

    def ring(c, d, to, half=None, own=False):
        put(c, d, ring_rows(c, half), 0 if half is None else half, (grp, to), own)

    def over(c, d):
        put(c, d, ring_rows(c), 0, (grp, partner))
        half = SIDE[c] // 2
        first = par * (ROWS - SIDE[c])
        put(c, d, (first, half), 2, (y_up, dev))
        put(c, d, (first + half, half), 3, (y_down, dev))

    def await_rows(d, span, sem):
        copy(d, *span, sem, (grp, partner)).wait_recv()

    def await_ring(c, d, half=None):
        await_rows(d, ring_rows(c, half), 0 if half is None else half)

    def take(src, base, d):
        @pl.loop(0, 4)
        def _(i):
            a = pl.multiple_of(base + i * 128, 128)
            b = pl.multiple_of(d * U_ROWS + i * 128, 128)
            utab[pl.ds(b, 128), :] = src[pl.ds(a, 128), :].astype(jnp.float32)

        v = src[pl.ds(pl.multiple_of(base + U_ROWS, 128), 128), :].astype(jnp.float32)
        r = pltpu.roll(v, 64, 1)
        a = pl.multiple_of(2 * d * S_ROWS, 128)
        stab[pl.ds(a, 128), :] = jnp.where(lane < 64, v, r)
        stab[pl.ds(a + 128, 128), :] = jnp.where(lane < 64, r, v)

    def own_shard(c):
        for to in (zp, zm, xp, xm) + ((x_far,) if c == 0 else ()):
            ring(c, dev, to, own=True)
        put(c, dev, (0, ROWS), 0, (grp, partner), own=True)

    def arrive(c, kind, dz, dx):
        d = at(dz, dx, c)
        if kind == "end":
            await_ring(c, d, 0)
            await_ring(c, d, 1)
        else:
            await_ring(c, d)
        if kind == "z":
            side = 0 if dz < 0 else 1
            ring(c, d, (zp, zm)[side], half=side if abs(dz) == 3 else None)
        if c == 0 and kind == "x":
            ring(c, d, zp)
            ring(c, d, zm)
        if c == 1 and dx == 0:
            ring(c, d, xp)
            ring(c, d, xm)
        if c == 1 and kind == "x":
            side = 0 if dx == 3 else 1
            ring(c, d, (xp, xm)[side], half=side)
        over(c, d)

    def arrive_y(c, dz, dx):
        d = at(dz, dx, c)
        half = SIDE[c] // 2
        first = (1 - par) * (ROWS - SIDE[c])
        await_rows(d, (first, half), 2)
        await_rows(d, (first + half, half), 3)
        put(c, d, (first, 2 * half), 2, (grp, partner))
        take(buf, d * ROWS, d)

    def arrive_partner(c, dz, dx):
        d = at(dz, dx, 1 - c)
        if dz == 0 and dx == 0:
            await_rows(d, (0, ROWS), 0)
        else:
            await_ring(1 - c, d)
            await_rows(d, ((1 - par) * (ROWS - SIDE[1 - c]), SIDE[1 - c]), 2)
        take(buf, d * ROWS, d)

    def masks(t):
        a = jnp.broadcast_to(v0_ref[pl.ds(t, 1), :], (128, 128))
        b = jnp.broadcast_to(v1_ref[pl.ds(t, 1), :], (128, 128))
        sv[pl.ds(pl.multiple_of(t * NZ, 128), 128), :] = jnp.where(sublane < 64, a, b).T

    def x_copy(src, dst, way, to):
        return pltpu.make_async_remote_copy(
            src_ref=src, dst_ref=dst, send_sem=send_x.at[way], recv_sem=recv_x.at[way],
            device_id=to, device_id_type=MESH,
        )

    def x_first(out, mid, way):
        for i in range(1, 8):
            zt = (z + i) % 8
            src = out.at[pl.ds(pl.multiple_of(zt * 32, 32), 32), :]
            dst = mid.at[pl.ds(pl.multiple_of(z * 40, 8), 32), :]
            x_copy(src, dst, way, (grp, zt * 8 + dev % 8)).start()
        mid[pl.ds(pl.multiple_of(z * 40, 8), 32), :] = out[pl.ds(pl.multiple_of(z * 32, 32), 32), :]

    def x_wait(buf, rows, way):
        ref = buf.at[pl.ds(0, rows), :]
        x_copy(ref, ref, way, (grp, partner)).wait_recv()

    def x_second(mid, turn, into, way):
        x_wait(mid, 224, way)
        for q in range(32):
            turn[q * 8 : q * 8 + 8, :] = mid[pl.ds(q, 8, stride=40), :]
        for i in range(1, 32):
            q = (quad + i) % 32
            src = turn.at[pl.ds(pl.multiple_of(q * 8, 8), 8), :]
            dst = into.at[pl.ds(pl.multiple_of(quad * 8, 8), 8), :]
            x_copy(src, dst, way + 1, in_plane(q)).start()
        own = pl.ds(pl.multiple_of(quad * 8, 8), 8)
        into[own, :] = turn[own, :]

    def x_sent(buf, way):
        for w, rows in ((way, 224), (way + 1, 248)):
            ref = buf.at[pl.ds(0, rows), :]
            x_copy(ref, ref, w, (grp, partner)).wait_send()

    def routing():
        local_copies[0].wait()
        local_copies[1].wait()
        lane1 = lax.broadcasted_iota(jnp.int32, (1, 128), 1)

        def look(i, row):
            for j in range(8):
                t = i * 8 + j
                row = jnp.where(lane1 == t, owner_s[word_s[t]], row)
            return row

        row = lax.fori_loop(0, NT // 8, look, jnp.zeros((1, 128), jnp.int32))
        across = jnp.broadcast_to(row, (128, 128))
        down = across.T
        same = (down // 64 == across // 64) & (sublane < lane)
        place = jnp.sum(same.astype(jnp.float32), axis=0, keepdims=True)
        owner = row // 64
        to = (owner // 8) % 8 * 32 + owner // 64 * 8 + owner % 8
        dest = lax.broadcasted_iota(jnp.int32, (256, 128), 0)
        far = owner != me
        ids = (down % 64 + 1).astype(jnp.bfloat16)
        found = []
        for p in range(CAP):
            hit = (to == dest) & far & (place == p)
            table = hit.astype(jnp.float32).astype(jnp.bfloat16)
            slots[p * 256 : (p + 1) * 256, :] = table
            found.append(jnp.dot(table, ids, preferred_element_type=jnp.float32))
        lane_w = lax.broadcasted_iota(jnp.int32, (256, 128), 1)
        id_out[...] = jnp.where(lane_w < 64, found[0], found[1]) - 1.0
        own = (down // 64 == me) & (down % 64 == lane)
        slots[512:640, :] = own.astype(jnp.float32).astype(jnp.bfloat16)

    def thirds(v):
        hi = v.astype(jnp.bfloat16)
        rest = v - hi.astype(jnp.float32)
        mid = rest.astype(jnp.bfloat16)
        low = (rest - mid.astype(jnp.float32)).astype(jnp.bfloat16)
        return hi, mid, low

    for c in (0, 1):
        pl.when(core == c)(functools.partial(own_shard, c))

    routing()
    x_first(id_out, id_mid, 0)
    take(own_in, 0, dev)

    def gather(c):
        mine = ORDER[c]
        theirs = (("", 0, 0),) + ORDER[1 - c]
        for i in range(31 + LAG_PARTNER + 1):
            if i < 31:
                arrive(c, *mine[i])

                @pl.loop(4 * i, 4 * i + 4)
                def _(t):
                    masks(t)

            if 0 <= i - LAG_Y < 31:
                arrive_y(c, *mine[i - LAG_Y][1:])
            if i - LAG_PARTNER >= 0:
                arrive_partner(c, *theirs[i - LAG_PARTNER][1:])

    for c in (0, 1):
        pl.when(core == c)(functools.partial(gather, c))
    assert sent_rows[0] == sent_rows[1] <= DEVS * ROWS

    x_second(id_mid, id_turn, id_in, 0)

    @pl.loop(124, NT)
    def _(t):
        masks(t)

    for c in local_copies[2:]:
        c.wait()
    ks = [kc_s[j] for j in range(8)]

    @pl.loop(0, NT)
    def _(t):
        def at_slot(index, n):
            return pl.ds(index.at[pl.ds(t, 1), pl.ds(n // 8 * 8, 8)][0, ks[n % 8]], 1)

        for n in range(NZ):
            g[n : n + 1, :] = stab[at_slot(srow_s, n), :]
        accs = [jnp.zeros((1, 128), jnp.float32) for _ in range(4)]
        for n in range(NZ):
            product = utab[at_slot(urow_s, n), :] * g[n : n + 1, :]
            accs[n % 4] = accs[n % 4] + product * sv[pl.ds(t * NZ + n, 1), :]
        sums[pl.ds(t, 1), :] = (accs[0] + accs[1]) + (accs[2] + accs[3])

    total = sums[...]
    total = total + pltpu.roll(total, 64, 1)
    parts = thirds(total)
    lane_w = lax.broadcasted_iota(jnp.int32, (256, 128), 1)
    picked = []
    for p in range(CAP):
        table = slots[p * 256 : (p + 1) * 256, :]
        hi, mid, low = (jnp.dot(table, v, preferred_element_type=jnp.float32) for v in parts)
        picked.append((hi + mid) + low)
    row_out[...] = jnp.where(lane_w < 64, picked[0], picked[1])
    x_first(row_out, row_mid, 2)

    def collect(table, v):
        hi, mid, low = (
            lax.dot_general(w, table, (((0,), (0,)), ((), ())), preferred_element_type=jnp.float32)
            for w in thirds(v)
        )
        return (hi + mid) + low

    own_part = collect(slots[512:640, :], total)
    x_wait(id_in, 248, 1)
    hits = (id_in[...] == (lane_w % 64).astype(jnp.float32)).astype(jnp.float32).astype(jnp.bfloat16)
    copy(0, 0, sent_rows[0], 0, (grp, partner)).wait_send()
    x_sent(id_out, 0)
    x_second(row_mid, row_turn, row_in, 2)
    x_wait(row_in, 248, 3)
    far_part = collect(hits, row_in[...])
    out_ref[...] = (own_part[:64, :64] + far_part[:64, :64]) + far_part[64:, 64:]
    x_sent(row_out, 2)


def shards(nz_user, nz_sub, nz_value, tile_word, word_owner, user_factor, sub_factor):
    f32, i32, bf16 = jnp.float32, jnp.int32, jnp.bfloat16
    kc = jnp.arange(128, dtype=i32)
    vmem = pl.BlockSpec(memory_space=pltpu.VMEM)
    hbm = pl.BlockSpec(memory_space=pl.ANY)
    rows = pltpu.VMEM((256, LANES), f32)
    return pl.pallas_call(
        kernel,
        out_shape=jax.ShapeDtypeStruct((64, 64), f32),
        in_specs=[hbm, hbm, hbm, hbm, vmem, vmem, vmem, vmem],
        out_specs=vmem,
        scratch_shapes=[
            pltpu.VMEM((DEVS * ROWS, LANES), bf16),
            pltpu.VMEM((DEVS * U_ROWS, LANES), f32),
            pltpu.VMEM((DEVS * S_ROWS * 2, LANES), f32),
            pltpu.VMEM((NT * NZ, LANES), f32),
            pltpu.VMEM((NZ, LANES), f32),
            pltpu.VMEM((ROWS, LANES), bf16),
            pltpu.VMEM((NT, NZ), i32),
            pltpu.VMEM((NT, NZ), f32),
            pltpu.VMEM((NT, NZ), f32),
            pltpu.VMEM((NT, LANES), f32),
            rows, pltpu.VMEM((320, LANES), f32), rows, rows,
            rows, pltpu.VMEM((320, LANES), f32), rows, rows,
            pltpu.VMEM((640, LANES), bf16),
            pltpu.SMEM((128,), i32),
            pltpu.SMEM((NT,), i32),
            pltpu.SMEM((16384,), i32),
            pltpu.SMEM((NT, NZ), i32),
            pltpu.SMEM((NT, NZ), i32),
            pltpu.SemaphoreType.DMA,
            pltpu.SemaphoreType.DMA((DEVS, 4)),
            pltpu.SemaphoreType.DMA((5,)),
            pltpu.SemaphoreType.DMA((4,)),
            pltpu.SemaphoreType.DMA((4,)),
        ],
        compiler_params=pltpu.CompilerParams(
            collective_id=0, has_side_effects=True, vmem_limit_bytes=58 * 2**20
        ),
    )(kc, tile_word, word_owner, nz_sub, nz_user, nz_value, user_factor, sub_factor)


def solution(mesh):
    return jax.shard_map(
        shards,
        mesh=mesh,
        in_specs=(
            P(("grp", "dev"), None),
            P(("grp", "dev"), None),
            P(("grp", "dev"), None),
            P(("grp", "dev")),
            P(),
            P(None, "dev"),
            P(None, "dev"),
        ),
        out_specs=P(None, ("grp", "dev")),
        check_vma=False,
    )
```
